32 devices in a mesh: grp: 2 (over y), theta: 8 (over z, x), phi: 2 (over core).
Axes of the slice: x: 2, y: 2, z: 4, core: 2. Of those that a mesh axis runs over, the one named last changes fastest.
Arguments:
- maps: bfloat16 [8, 4096, 4096], P('grp', 'theta', 'phi'), parts along dimension 0, may hold values from -6 to 6
- deltas: bfloat16 [4096, 4, 4096], P('phi', None, 'theta'), may hold values from -1 to 1
- spin_rows: bfloat16 [4096, 2, 4], P('phi'), may hold values from -1 to 1
- ell_index: int32 [4], replicated, may hold values from 1024 to 2047
- owner_map: int32 [4096], replicated, may hold values from 0 to 4095, each once
- prior: float32 [4], replicated, may hold values from 0.3 to 3
Outputs:
- gradient: float32 [8, 2, 4096], P('grp', None, ('theta', 'phi')), parts along dimension 0
The draws below stay inside these ranges and needn't reach their ends.
There are 2 independent parts, one for each index of `grp`. The reference program is written for one: setup_inputs(seed, part) draws one part's arguments, and reference() takes and returns one part's arrays. A program takes and returns all parts, laid end to end along the dimension named above; an argument that names none is the same for every part. Nothing has to cross between parts.
Inputs may be any that keep to these rules, and one draw needn't show every extreme that they name: `ell_index`: every selected degree is at least 1024; tables may repeat a degree. A permutation of the Fourier indices; slot s of deltas and of the output belongs to the frequency owner_map[s].
All inputs are finite; a program needn't handle non-finite values.
Results may differ from the reference program's by a relative error of at most 0.0003.
Values may be sent and summed in bfloat16 or wider, within the bound.
A program may use at most 256 MiB of HBM per device.

```python
import math
import jax
import jax.numpy as jnp
from jax import lax

L = 2048
NL = 4


def touch_ends(result, rng, low, top_value):
    place = [jax.random.randint(jax.random.fold_in(rng, axis), (), 0, length) for axis, length in enumerate(result.shape)]
    longest = result.shape.index(max(result.shape))
    beside = place[:longest] + [(place[longest] + 1) % result.shape[longest]] + place[longest + 1:]
    return result.at[tuple(place)].set(low).at[tuple(beside)].set(top_value)


def shard_levels(rng, dims, shards, low, high):
    factor_of, own = 1.0, jax.random.fold_in(rng, 6)
    for dim, parts in shards:
        steps = jnp.exp(jax.random.uniform(jax.random.fold_in(own, dim), (parts,), jnp.float32, low / len(shards), high / len(shards)))
        factor_of = factor_of * jnp.repeat(steps, dims[dim] // parts).reshape([-1 if axis == dim else 1 for axis in range(len(dims))])
    return factor_of


def bell_draw(rng, dims, width, limit, pieces=(), kind=jnp.bfloat16):
    array = width * jax.random.normal(rng, dims, jnp.float32)
    if pieces:
        array = array * shard_levels(rng, dims, pieces, -0.22, 0.18)
    return jnp.clip(array, -limit, limit).astype(kind)


def setup_inputs(seed: int = 0, part: int = 0) -> dict:
    streams_of = jax.random.split(jax.random.key(seed), 7)
    part_keys = jax.random.split(jax.random.fold_in(streams_of[6], part), 7)
    maps = bell_draw(part_keys[0], (4, 2 * L, 2 * L), 1.0, 6.0, ((1, 8), (2, 2)))
    deltas = jnp.clip(jax.random.uniform(streams_of[1], (2 * L, NL, 2 * L), jnp.float32, -1.0, 1.0) * shard_levels(streams_of[1], (2 * L, NL, 2 * L), ((0, 2), (2, 8)), -0.4, 0.0), -1.0, 1.0).astype(jnp.bfloat16)
    spin_rows = jnp.clip(jax.random.uniform(streams_of[2], (2 * L, 2, NL), jnp.float32, -1.0, 1.0) * shard_levels(streams_of[2], (2 * L, 2, NL), ((0, 2),), -0.4, 0.0), -1.0, 1.0).astype(jnp.bfloat16)
    ell_index = touch_ends(jax.random.randint(streams_of[3], (NL,), L // 2, L), jax.random.fold_in(streams_of[3], 1), L // 2, L - 1).astype(jnp.int32)
    owner_map = jax.random.permutation(streams_of[4], 2 * L).astype(jnp.int32)
    prior = jnp.clip(jnp.exp(jax.random.uniform(streams_of[5], (NL,), jnp.float32, math.log(0.3), math.log(3.0))), 0.3, 3.0)
    return dict(maps=maps, deltas=deltas, spin_rows=spin_rows, ell_index=ell_index, owner_map=owner_map, prior=prior)


def signed_freq(length):
    positions = jnp.arange(length, dtype=jnp.int32)
    return jnp.where(positions < length // 2, positions, positions - length)

def reference(maps, deltas, spin_rows, ell_index, owner_map, prior):
    length = 2 * L
    values = maps.astype(jnp.float32)
    prod_real = values[1] * values[2]
    prod_imag = values[1] * values[3]
    scalar_spec = jnp.fft.fft2(values[0]) / length
    spin_spec = jnp.fft.fft2(lax.complex(prod_real, prod_imag)) / length
    planes = [jnp.real(scalar_spec)[:, owner_map].astype(jnp.float32), jnp.imag(scalar_spec)[:, owner_map].astype(jnp.float32), jnp.real(spin_spec)[:, owner_map].astype(jnp.float32), jnp.imag(spin_spec)[:, owner_map].astype(jnp.float32)]
    freq = signed_freq(length)
    slot_freq = freq[owner_map]
    turns = jnp.mod(-slot_freq, 4)
    phase_real = jnp.where(turns == 0, 1.0, jnp.where(turns == 2, -1.0, 0.0)).astype(jnp.float32)
    phase_imag = jnp.where(turns == 1, 1.0, jnp.where(turns == 3, -1.0, 0.0)).astype(jnp.float32)
    outputs = []
    for degree in range(NL):
        ell = ell_index[degree]
        ell_float = ell.astype(jnp.float32)
        keep_rows = (jnp.abs(freq) <= ell).astype(jnp.float32)
        keep_slots = (jnp.abs(slot_freq) <= ell).astype(jnp.float32)
        table = deltas[:, degree, :].astype(jnp.float32)
        weight = 2.0 * math.pi / length * jnp.sqrt((2.0 * ell_float + 1.0) / (4.0 * math.pi))
        sums = []
        for plane_pos in range(4):
            spin = plane_pos // 2
            row_weights = spin_rows[:, spin, degree].astype(jnp.float32) * keep_rows
            total = jnp.einsum('k,ks->s', row_weights, table * planes[plane_pos], precision=lax.Precision.HIGHEST)
            sums.append(total * weight * keep_slots)
        coupling = prior[degree] * jnp.sqrt(ell_float * (ell_float + 1.0)) / L
        inner_real = -sums[3] - coupling * sums[0]
        inner_imag = sums[2] - coupling * sums[1]
        out_real = phase_real * inner_real - phase_imag * inner_imag
        out_imag = phase_real * inner_imag + phase_imag * inner_real
        outputs.append(jnp.stack([out_real, out_imag]))
    return jnp.stack(outputs)
```

```python
import functools
import math

import jax
import jax.numpy as jnp
from jax import lax
from jax.experimental import pallas as pl
from jax.experimental.pallas import tpu as pltpu
from jax.sharding import PartitionSpec as P


def exact_einsum(form, table, operand):
    return jnp.einsum(form, table, operand, precision=lax.Precision.HIGHEST)


def angle_tables(row_count, start, count, modulus):
    freq_rows = jnp.arange(row_count, dtype=jnp.int32)
    sample_cols = start + jnp.arange(count, dtype=jnp.int32)
    angles = (
        2.0
        * math.pi
        / modulus
        * jnp.mod(freq_rows[:, None] * sample_cols[None, :], modulus).astype(jnp.float32)
    )
    return (jnp.cos(angles), jnp.sin(angles))


def row_transform(real_part, imag_part, outer_len, inner_len):
    row_count = real_part.shape[0]
    length = outer_len * inner_len
    cos_a, sin_a = angle_tables(outer_len, 0, outer_len, outer_len)
    real_blocks = real_part.reshape(row_count, outer_len, inner_len)
    section_real = exact_einsum("ka,rab->rkb", cos_a, real_blocks)
    section_imag = -exact_einsum("ka,rab->rkb", sin_a, real_blocks)
    if imag_part is not None:
        imag_blocks = imag_part.reshape(row_count, outer_len, inner_len)
        section_real = section_real + exact_einsum("ka,rab->rkb", sin_a, imag_blocks)
        section_imag = section_imag + exact_einsum("ka,rab->rkb", cos_a, imag_blocks)
    cos_t, sin_t = angle_tables(outer_len, 0, inner_len, length)
    turned_real = section_real * cos_t + section_imag * sin_t
    turned_imag = section_imag * cos_t - section_real * sin_t
    cos_b, sin_b = angle_tables(inner_len, 0, inner_len, inner_len)
    out_real = exact_einsum("qb,rkb->rqk", cos_b, turned_real) + exact_einsum(
        "qb,rkb->rqk", sin_b, turned_imag
    )
    out_imag = exact_einsum("qb,rkb->rqk", cos_b, turned_imag) - exact_einsum(
        "qb,rkb->rqk", sin_b, turned_real
    )
    return (out_real.reshape(row_count, length), out_imag.reshape(row_count, length))


def column_transform(real_part, imag_part, outer_len, inner_len, start):
    fields = real_part.shape[0]
    count = real_part.shape[2]
    slots = real_part.shape[3]
    length = outer_len * inner_len
    cos_a, sin_a = angle_tables(outer_len, 0, outer_len, outer_len)
    section_real = exact_einsum("ka,fabm->fkbm", cos_a, real_part) + exact_einsum(
        "ka,fabm->fkbm", sin_a, imag_part
    )
    section_imag = exact_einsum("ka,fabm->fkbm", cos_a, imag_part) - exact_einsum(
        "ka,fabm->fkbm", sin_a, real_part
    )
    cos_t, sin_t = angle_tables(outer_len, start, count, length)
    cos_t = cos_t[:, :, None]
    sin_t = sin_t[:, :, None]
    turned_real = section_real * cos_t + section_imag * sin_t
    turned_imag = section_imag * cos_t - section_real * sin_t
    cos_b, sin_b = angle_tables(inner_len, start, count, inner_len)
    out_real = exact_einsum("qb,fkbm->fqkm", cos_b, turned_real) + exact_einsum(
        "qb,fkbm->fqkm", sin_b, turned_imag
    )
    out_imag = exact_einsum("qb,fkbm->fqkm", cos_b, turned_imag) - exact_einsum(
        "qb,fkbm->fqkm", sin_b, turned_real
    )
    return (out_real.reshape(fields, length, slots), out_imag.reshape(fields, length, slots))


def accumulate(spectrum_block, table_block, spin_block, length, ell_index):
    count = table_block.shape[0]
    positions = jnp.arange(count, dtype=jnp.int32)
    freq = jnp.where(positions < length // 2, positions, positions - length)
    terms = []
    for degree in range(table_block.shape[1]):
        keep_rows = (jnp.abs(freq) <= ell_index[degree]).astype(jnp.float32)
        row_weights = spin_block[:, :, degree].astype(jnp.float32).T * keep_rows[None, :]
        table = table_block[:, degree, :].astype(jnp.float32)
        terms.append(
            jnp.einsum(
                "fk,ks,xfks->fxs",
                row_weights,
                table,
                spectrum_block,
                precision=lax.Precision.HIGHEST,
            )
        )
    return jnp.stack(terms)


def on_device_general(maps, deltas, spin_rows, ell_index, owner_map, prior):
    theta_count = lax.axis_size("theta")
    phi_count = lax.axis_size("phi")
    length = maps.shape[2] * phi_count
    values = maps.astype(jnp.float32)
    planes = jnp.stack([values[0], values[1] * values[2], values[1] * values[3]])
    row_planes = lax.all_to_all(planes, "phi", split_axis=1, concat_axis=2, tiled=True)
    inner_len = length // theta_count
    spectra = [
        row_transform(row_planes[0], None, theta_count, inner_len),
        row_transform(row_planes[1], row_planes[2], theta_count, inner_len),
    ]
    stacked = jnp.stack(
        [
            jnp.stack([spectrum[0] for spectrum in spectra]),
            jnp.stack([spectrum[1] for spectrum in spectra]),
        ]
    )
    permuted = jnp.take(stacked, owner_map, axis=3)
    columns = lax.all_to_all(permuted, "theta", split_axis=3, concat_axis=2, tiled=True)
    fields = columns.shape[1]
    slots = columns.shape[3]
    sub_rows = columns.shape[2] // theta_count
    blocks = columns.reshape(2, fields, theta_count, sub_rows, slots)
    row_start = lax.axis_index("phi") * sub_rows
    spec_real, spec_imag = column_transform(blocks[0], blocks[1], theta_count, inner_len, row_start)
    combined = jnp.stack([spec_real, spec_imag])
    totals = accumulate(
        combined,
        lax.all_gather(deltas, "phi", axis=0, tiled=True),
        lax.all_gather(spin_rows, "phi", axis=0, tiled=True),
        length,
        ell_index,
    )
    shares = lax.psum_scatter(totals, "phi", scatter_dimension=3, tiled=True)
    share_count = shares.shape[3]
    slot_start = lax.axis_index("theta") * slots + lax.axis_index("phi") * share_count
    share_ids = lax.dynamic_slice_in_dim(owner_map, slot_start, share_count)
    slot_freq = jnp.where(share_ids < length // 2, share_ids, share_ids - length)
    ell_float = ell_index.astype(jnp.float32)
    weight = 2.0 * math.pi / length * jnp.sqrt((2.0 * ell_float + 1.0) / (4.0 * math.pi)) / length
    keep_slots = (jnp.abs(slot_freq)[None, :] <= ell_index[:, None]).astype(jnp.float32) * weight[
        :, None
    ]
    scalar_real = shares[:, 0, 0] * keep_slots
    scalar_imag = shares[:, 0, 1] * keep_slots
    spin_real = shares[:, 1, 0] * keep_slots
    spin_imag = shares[:, 1, 1] * keep_slots
    coupling = (prior * jnp.sqrt(ell_float * (ell_float + 1.0)) / (length // 2))[:, None]
    inner_real = -spin_imag - coupling * scalar_real
    inner_imag = spin_real - coupling * scalar_imag
    turns = jnp.mod(-slot_freq, 4)
    phase_real = jnp.where(turns == 0, 1.0, jnp.where(turns == 2, -1.0, 0.0)).astype(jnp.float32)[
        None, :
    ]
    phase_imag = jnp.where(turns == 1, 1.0, jnp.where(turns == 3, -1.0, 0.0)).astype(jnp.float32)[
        None, :
    ]
    out_real = phase_real * inner_real - phase_imag * inner_imag
    out_imag = phase_real * inner_imag + phase_imag * inner_real
    return jnp.stack([out_real, out_imag], axis=1)


ROW_OUTER = 8
VMEM_LIMIT = 60 * 1024 * 1024
CODE_TOP = 32767.0


def cplx_add(x, y):
    return tuple(b if a is None else a if b is None else a + b for a, b in zip(x, y))


def cplx_sub(x, y):
    return tuple(
        (None if b is None else -b) if a is None else a if b is None else a - b
        for a, b in zip(x, y)
    )


def turn(x, step, count):
    real, imag = x
    if step == 0:
        return x
    if 4 * step == count:
        return (imag, None if real is None else -real)
    cos_v = math.cos(2.0 * math.pi * step / count)
    sin_v = math.sin(2.0 * math.pi * step / count)
    if imag is None:
        return (real * cos_v, real * -sin_v)
    if 8 * step == count:
        return ((real + imag) * cos_v, (imag - real) * cos_v)
    if 8 * step == 3 * count:
        return ((imag - real) * sin_v, (real + imag) * -sin_v)
    return (real * cos_v + imag * sin_v, imag * cos_v - real * sin_v)


def butterfly(items):
    count = len(items)
    if count == 1:
        return items
    even, odd = butterfly(items[::2]), butterfly(items[1::2])
    turned = [turn(x, step, count) for step, x in enumerate(odd)]
    return [cplx_add(a, b) for a, b in zip(even, turned)] + [
        cplx_sub(a, b) for a, b in zip(even, turned)
    ]


def split_store(high, low, where, value):
    top = value.astype(jnp.bfloat16)
    high[where] = top
    low[where] = (value - top.astype(jnp.float32)).astype(jnp.bfloat16)


def store_matrix(cos_ref, sin_ref, high, low):
    size = cos_ref.shape[0]
    first, second = slice(0, size), slice(size, 2 * size)
    cos_v, sin_v = cos_ref[...], sin_ref[...]
    split_store(high, low, (first, first), cos_v)
    split_store(high, low, (first, second), sin_v)
    split_store(high, low, (second, first), -sin_v)
    split_store(high, low, (second, second), cos_v)


def store_turned(high, low, k, rows, item, cos_t, sin_t):
    real, imag = item
    size = real.shape[1]
    cos_k, sin_k = cos_t[k : k + 1, :], sin_t[k : k + 1, :]
    if imag is None:
        out_real, out_imag = real * cos_k, real * -sin_k
    else:
        out_real, out_imag = real * cos_k + imag * sin_k, imag * cos_k - real * sin_k
    split_store(high, low, (k, rows, slice(0, size)), out_real)
    split_store(high, low, (k, rows, slice(size, 2 * size)), out_imag)


def dot_nt(left, right):
    return lax.dot_general(
        left, right, (((1,), (1,)), ((), ())), preferred_element_type=jnp.float32
    )


def three_dots(mat_high, mat_low, x_high, x_low, k):
    high = x_high[k]
    return (
        dot_nt(mat_high[...], high) + dot_nt(mat_high[...], x_low[k]) + dot_nt(mat_low[...], high)
    )


def row_kernel(kept, *refs):
    planes = refs[:-10]
    cos_b, sin_b, cos_t, sin_t, code_ref, scale_ref, mat_high, mat_low, x_high, x_low = refs[-10:]
    k = pl.program_id(0)
    inner = cos_b.shape[0]

    @pl.when(k == 0)
    def _():
        store_matrix(cos_b, sin_b, mat_high, mat_low)
        step_rows = 16

        def chunk(step, carry):
            rows = pl.ds(pl.multiple_of(step * step_rows, step_rows), step_rows)

            def part(ref, a):
                return ref[0, rows, a * inner : (a + 1) * inner].astype(jnp.float32)

            items = []
            for a in range(ROW_OUTER):
                if len(planes) == 1:
                    items.append((part(planes[0], a), None))
                else:
                    base = part(planes[0], a)
                    items.append((base * part(planes[1], a), base * part(planes[2], a)))
            done = butterfly(items)
            for out in range(kept):
                store_turned(x_high, x_low, out, rows, done[out], cos_t, sin_t)
            return carry

        lax.fori_loop(0, planes[0].shape[1] // step_rows, chunk, 0)

    both = three_dots(mat_high, mat_low, x_high, x_low, k)
    real, imag = both[:inner], both[inner:]
    top = jnp.max(jnp.maximum(jnp.abs(real), jnp.abs(imag)), axis=1, keepdims=True)
    top = jnp.maximum(top, 1e-30)
    factor = CODE_TOP / top
    code_real = jnp.round(real * factor).astype(jnp.int32)
    code_imag = jnp.round(imag * factor).astype(jnp.int32)
    code_ref[0] = (code_real << 16) | (code_imag & 0xFFFF)
    scale_ref[0] = jnp.broadcast_to(top * (1.0 / CODE_TOP), (inner, 128))


def row_call(maps, places, kept, cos_b, sin_b, cos_t, sin_t):
    rows, length = maps.shape[1:]
    inner = cos_b.shape[0]
    whole = lambda shape: pl.BlockSpec(shape, lambda k: (0, 0))
    plane = lambda place: pl.BlockSpec((1, rows, length), lambda k: (place, 0, 0))
    return pl.pallas_call(
        functools.partial(row_kernel, kept),
        grid=(kept,),
        in_specs=[plane(place) for place in places]
        + [whole(cos_b.shape), whole(sin_b.shape), whole(cos_t.shape), whole(sin_t.shape)],
        out_specs=[
            pl.BlockSpec((1, inner, rows), lambda k: (k, 0, 0)),
            pl.BlockSpec((1, inner, 128), lambda k: (k, 0, 0)),
        ],
        out_shape=[
            jax.ShapeDtypeStruct((kept, inner, rows), jnp.int32),
            jax.ShapeDtypeStruct((kept, inner, 128), jnp.float32),
        ],
        scratch_shapes=[
            pltpu.VMEM((2 * inner, 2 * inner), jnp.bfloat16),
            pltpu.VMEM((2 * inner, 2 * inner), jnp.bfloat16),
            pltpu.VMEM((kept, rows, 2 * inner), jnp.bfloat16),
            pltpu.VMEM((kept, rows, 2 * inner), jnp.bfloat16),
        ],
        compiler_params=pltpu.CompilerParams(vmem_limit_bytes=VMEM_LIMIT),
        cost_estimate=pl.CostEstimate(
            flops=24 * kept * inner * inner * rows,
            bytes_accessed=len(places) * rows * length * 2 + kept * inner * (rows + 128) * 4,
            transcendentals=0,
        ),
    )(*([maps] * len(places)), cos_b, sin_b, cos_t, sin_t)


def column_kernel(
    code_ref, sre_ref, sim_ref, table_ref, row_w, cos_b, sin_b, cos_t, sin_t, out_ref,
    mat_high, mat_low, x_high, x_low, total,
):
    k = pl.program_id(0)
    outer = code_ref.shape[0]
    slots = code_ref.shape[1]
    inner = code_ref.shape[2]
    degrees = table_ref.shape[1]

    @pl.when(k == 0)
    def _():
        store_matrix(cos_b, sin_b, mat_high, mat_low)
        total[...] = jnp.zeros_like(total)
        step_rows = 16

        def chunk(step, carry):
            rows = pl.ds(pl.multiple_of(step * step_rows, step_rows), step_rows)
            sre, sim = sre_ref[rows, :], sim_ref[rows, :]
            items = []
            for a in range(outer):
                code = code_ref[a, rows, :]
                real = (code >> 16).astype(jnp.float32) * sre[:, a : a + 1]
                imag = ((code << 16) >> 16).astype(jnp.float32) * sim[:, a : a + 1]
                items.append((real, imag))
            for out, item in enumerate(butterfly(items)):
                store_turned(x_high, x_low, out, rows, item, cos_t, sin_t)
            return carry

        lax.fori_loop(0, slots // step_rows, chunk, 0)

    both = three_dots(mat_high, mat_low, x_high, x_low, k)
    real, imag = both[:inner], both[inner:]
    for degree in range(degrees):
        weighted = table_ref[0, degree].astype(jnp.float32) * row_w[0, :, degree : degree + 1]
        for part, value in enumerate((real, imag)):
            total[2 * degree + part] += jnp.sum(
                (weighted * value).reshape(inner // 8, 8, slots), axis=0
            )

    @pl.when(k == outer - 1)
    def _():
        out_ref[...] = jnp.sum(total[...], axis=1)


def column_call(codes, sre, sim, tables, row_w, cos_b, sin_b, cos_t, sin_t):
    outer, slots, inner = codes.shape
    degrees = tables.shape[1]
    whole = lambda shape: pl.BlockSpec(shape, lambda k: (0,) * len(shape))
    return pl.pallas_call(
        column_kernel,
        grid=(outer,),
        in_specs=[
            whole(codes.shape),
            whole(sre.shape),
            whole(sim.shape),
            pl.BlockSpec((1, degrees, inner, slots), lambda k: (k, 0, 0, 0)),
            pl.BlockSpec((1, inner, degrees), lambda k: (k, 0, 0)),
            whole(cos_b.shape),
            whole(sin_b.shape),
            whole(cos_t.shape),
            whole(sin_t.shape),
        ],
        out_specs=whole((2 * degrees, slots)),
        out_shape=jax.ShapeDtypeStruct((2 * degrees, slots), jnp.float32),
        scratch_shapes=[
            pltpu.VMEM((2 * inner, 2 * inner), jnp.bfloat16),
            pltpu.VMEM((2 * inner, 2 * inner), jnp.bfloat16),
            pltpu.VMEM((outer, slots, 2 * inner), jnp.bfloat16),
            pltpu.VMEM((outer, slots, 2 * inner), jnp.bfloat16),
            pltpu.VMEM((2 * degrees, 8, slots), jnp.float32),
        ],
        compiler_params=pltpu.CompilerParams(vmem_limit_bytes=VMEM_LIMIT),
        cost_estimate=pl.CostEstimate(
            flops=24 * outer * inner * inner * slots,
            bytes_accessed=outer * slots * inner * (4 + 2 * degrees),
            transcendentals=0,
        ),
    )(codes, sre, sim, tables, row_w, cos_b, sin_b, cos_t, sin_t)


def trig_tables(row_ids, col_ids, modulus):
    product = jnp.mod(row_ids[:, None] * col_ids[None, :], modulus)
    angles = (2.0 * math.pi / modulus) * product.astype(jnp.float32)
    return jnp.cos(angles), jnp.sin(angles)


def signed(ids, length):
    return jnp.where(ids < length // 2, ids, ids - length)


def on_device(maps, deltas, spin_rows, ell_index, owner_map, prior):
    owners = ("theta", "phi")
    phi_count = lax.axis_size("phi")
    length = maps.shape[2] * phi_count
    outer = lax.axis_size("theta") * phi_count
    sub_rows = length // outer
    slots = sub_rows
    row_inner = length // ROW_OUTER
    ids = lax.optimization_barrier(jnp.arange(length, dtype=jnp.int32))
    row_trig = trig_tables(ids[:row_inner], ids[:row_inner], row_inner) + trig_tables(
        ids[:ROW_OUTER], ids[:row_inner], length
    )
    col_trig = trig_tables(ids[:sub_rows], ids[:sub_rows], sub_rows) + trig_tables(
        ids[:outer], ids[:sub_rows], length
    )
    rows = lax.all_to_all(maps, "phi", split_axis=1, concat_axis=2, tiled=True)

    residue = owner_map % ROW_OUTER
    flipped = residue > ROW_OUTER // 2
    half_map = jnp.where(flipped, length - owner_map, owner_map)
    slot_start = (lax.axis_index("theta") * phi_count + lax.axis_index("phi")) * slots
    own = lambda array: lax.dynamic_slice_in_dim(array, slot_start, slots)
    own_ids = own(owner_map)

    def spectrum(places, kept, freq):
        codes, scales = row_call(rows, places, kept, *row_trig)
        place = (freq % ROW_OUTER) * row_inner + freq // ROW_OUTER
        table = codes.reshape(kept * row_inner, sub_rows)
        sorted_codes = table.at[place].get(mode="promise_in_bounds", unique_indices=False)
        received = lax.all_to_all(
            sorted_codes.reshape(outer, slots, sub_rows), owners, 0, 0, tiled=True
        )
        flat = lax.all_gather(scales[:, :, 0].reshape(-1), owners, axis=0)
        picks = (own(place)[:, None] == ids[None, : kept * row_inner]).astype(jnp.float32)
        own_scales = jnp.einsum("am,sm->sa", flat, picks, precision=lax.Precision.HIGHEST)
        return received, own_scales

    code_scalar, scale_scalar = spectrum((0,), ROW_OUTER // 2 + 1, half_map)
    code_spin, scale_spin = spectrum((1, 2, 3), ROW_OUTER, owner_map)

    tables = lax.all_to_all(deltas, "phi", split_axis=2, concat_axis=0, tiled=True)
    degrees = tables.shape[1]
    tables = tables.reshape(sub_rows, outer, degrees, slots).transpose(1, 2, 0, 3)
    spins = lax.all_gather(spin_rows, "phi", axis=0, tiled=True).astype(jnp.float32)
    keep_rows = jnp.abs(signed(ids, length))[:, None] <= ell_index[None, :]
    row_w = jnp.where(keep_rows[:, None, :], spins, 0.0)
    row_w = row_w.reshape(sub_rows, outer, 2, degrees).transpose(2, 1, 0, 3)

    mirror = jnp.where(own(flipped), -1.0, 1.0)[:, None]
    scalar = column_call(
        code_scalar, scale_scalar, scale_scalar * mirror, tables, row_w[0], *col_trig
    ).reshape(degrees, 2, slots)
    spin = column_call(
        code_spin, scale_spin, scale_spin, tables, row_w[1], *col_trig
    ).reshape(degrees, 2, slots)

    slot_freq = signed(own_ids, length)
    ell_float = ell_index.astype(jnp.float32)
    weight = 2.0 * math.pi / length * jnp.sqrt((2.0 * ell_float + 1.0) / (4.0 * math.pi)) / length
    keep = jnp.abs(slot_freq)[None, :] <= ell_index[:, None]
    keep_slots = keep.astype(jnp.float32) * weight[:, None]
    coupling = (prior * jnp.sqrt(ell_float * (ell_float + 1.0)) / (length // 2))[:, None]
    inner_real = (-spin[:, 1] - coupling * scalar[:, 0]) * keep_slots
    inner_imag = (spin[:, 0] - coupling * scalar[:, 1]) * keep_slots
    turns = jnp.mod(-slot_freq, 4)[None, :]
    phase_real = jnp.where(turns == 0, 1.0, jnp.where(turns == 2, -1.0, 0.0))
    phase_imag = jnp.where(turns == 1, 1.0, jnp.where(turns == 3, -1.0, 0.0))
    out_real = phase_real * inner_real - phase_imag * inner_imag
    out_imag = phase_real * inner_imag + phase_imag * inner_real
    return jnp.stack([out_real, out_imag], axis=1)


def solution(mesh):
    owner_count = mesh.shape["theta"] * mesh.shape["phi"]
    body = on_device if owner_count <= 16 else on_device_general
    placed = (
        P("grp", "theta", "phi"),
        P("phi", None, "theta"),
        P("phi", None, None),
        P(),
        P(),
        P(),
    )
    return jax.shard_map(
        body,
        mesh=mesh,
        in_specs=placed,
        out_specs=P("grp", None, ("theta", "phi")),
        check_vma=False,
    )
```
